16 devices in a mesh: row: 2 (over z), col: 8 (over y, x, core).
Axes of the slice: x: 2, y: 2, z: 2, core: 2. Of those that a mesh axis runs over, the one named last changes fastest.
Arguments:
- v_panels: float32 [4096, 4096], P('row', 'col')
- t_factors: float32 [128, 32, 32], replicated
- z_vecs: float32 [4096, 2048], P(None, ('col', 'row'))
- chol_low: float32 [4096, 4096], P('row', 'col')
Outputs:
- output: float32 [4096, 2048], P('row', 'col')
All inputs are finite; a program needn't handle non-finite values.
Results may differ from the reference program's by a relative error of at most 0.001.
Values sent between devices are 32-bit elements.
A program may use at most 1 GiB of HBM per device.

```python
import jax
import jax.numpy as jnp
from jax import lax

MAT_N = 4096
PANEL_W = 32
N_VECS = 2048
ROW_GRID = 2
COL_GRID = 8
NUM_PANELS = MAT_N // PANEL_W


def rows_to_stored(mat):
    n_cols = mat.shape[1]
    return mat.reshape(NUM_PANELS // ROW_GRID, ROW_GRID, PANEL_W, n_cols).transpose(1, 0, 2, 3).reshape(MAT_N, n_cols)


def rows_to_natural(mat):
    n_cols = mat.shape[1]
    return mat.reshape(ROW_GRID, NUM_PANELS // ROW_GRID, PANEL_W, n_cols).transpose(1, 0, 2, 3).reshape(MAT_N, n_cols)


def cols_to_stored(mat):
    return mat.reshape(MAT_N, NUM_PANELS // COL_GRID, COL_GRID, PANEL_W).transpose(0, 2, 1, 3).reshape(MAT_N, MAT_N)


def cols_to_natural(mat):
    return mat.reshape(MAT_N, COL_GRID, NUM_PANELS // COL_GRID, PANEL_W).transpose(0, 2, 1, 3).reshape(MAT_N, MAT_N)


def compact_factors(v_nat):
    v_blocks = v_nat.reshape(MAT_N, NUM_PANELS, PANEL_W).transpose(1, 0, 2)
    gram_mat = jnp.einsum('mnb,mnc->mbc', v_blocks, v_blocks)
    half_diag = jnp.eye(PANEL_W, dtype=v_nat.dtype) * 0.5
    t_inv = jnp.triu(gram_mat, 1) + gram_mat * half_diag
    return jnp.triu(jnp.linalg.inv(t_inv))


def setup_inputs(seed: int = 0) -> dict:
    base_key = jax.random.key(seed)
    key_v, key_z, key_l, key_d = jax.random.split(base_key, 4)
    row_ids = jnp.arange(MAT_N)[:, None]
    col_ids = jnp.arange(MAT_N)[None, :]
    top_rows = (col_ids // PANEL_W) * PANEL_W
    row_scale = jnp.where(row_ids < top_rows + PANEL_W, PANEL_W ** -0.5, 1.0)
    below_rand = jax.random.normal(key_v, (MAT_N, MAT_N), jnp.float32)
    v_nat = jnp.where(row_ids > col_ids, below_rand * row_scale, 0.0) + jnp.where(row_ids == col_ids, 1.0, 0.0)
    v_nat = v_nat.astype(jnp.float32)
    t_factors = compact_factors(v_nat).astype(jnp.float32)
    off_diag = jax.random.normal(key_l, (MAT_N, MAT_N), jnp.float32) * (0.5 * MAT_N ** -0.5)
    diag_vals = jax.random.uniform(key_d, (MAT_N,), jnp.float32, 0.5, 2.0)
    l_nat = (jnp.where(row_ids > col_ids, off_diag, 0.0) + jnp.diag(diag_vals)).astype(jnp.float32)
    z_vecs = jax.random.normal(key_z, (MAT_N, N_VECS), jnp.float32)
    return {'v_panels': rows_to_stored(cols_to_stored(v_nat)), 't_factors': t_factors, 'z_vecs': z_vecs, 'chol_low': rows_to_stored(cols_to_stored(l_nat))}


def reference(v_panels, t_factors, z_vecs, chol_low):
    v_nat = rows_to_natural(cols_to_natural(v_panels))
    l_nat = rows_to_natural(cols_to_natural(chol_low))
    x_start = rows_to_natural(z_vecs)
    v_blocks = v_nat.reshape(MAT_N, NUM_PANELS, PANEL_W).transpose(1, 0, 2)

    def apply_panel(x_mat, inputs):
        v_pan, t_pan = inputs
        w_mat = jnp.dot(v_pan.T, x_mat, preferred_element_type=jnp.float32)
        y_mat = jnp.dot(t_pan, w_mat, preferred_element_type=jnp.float32)
        return x_mat - jnp.dot(v_pan, y_mat, preferred_element_type=jnp.float32), None

    x_nat, _ = lax.scan(apply_panel, x_start, (v_blocks, t_factors), reverse=True)
    l_blocks = l_nat.reshape(MAT_N, NUM_PANELS, PANEL_W).transpose(1, 0, 2)

    def solve_block(y_mat, inputs):
        l_pan, blk_idx = inputs
        row_start = blk_idx * PANEL_W
        w_mat = jnp.dot(l_pan.T, y_mat, preferred_element_type=jnp.float32)
        rhs_blk = lax.dynamic_slice(x_nat, (row_start, 0), (PANEL_W, N_VECS)) - w_mat
        diag_blk = lax.dynamic_slice(l_pan, (row_start, 0), (PANEL_W, PANEL_W))
        sol_blk = lax.linalg.triangular_solve(diag_blk, rhs_blk, left_side=True, lower=True, transpose_a=True)
        return lax.dynamic_update_slice(y_mat, sol_blk, (row_start, 0)), None

    y_nat, _ = lax.scan(solve_block, jnp.zeros_like(x_nat), (l_blocks, jnp.arange(NUM_PANELS)), reverse=True)
    return rows_to_stored(y_nat)
```

```python
import functools

import jax
import jax.numpy as jnp
from jax import lax
from jax.experimental import pallas as pl
from jax.experimental.pallas import tpu as pltpu
from jax.sharding import PartitionSpec as P

HI = lax.Precision.HIGHEST
MESH = pl.DeviceIdType.MESH
F32 = jnp.float32

PW = 32
NR = 16
NTILE = NR * (NR + 1) // 2
PARTS = 3
PART_LANES = 256
CHUNK_TILES = PARTS * PART_LANES // 128
CHUNK_LANES = CHUNK_TILES * 128
NCH = -(-2 * NTILE // CHUNK_TILES)
LANES = NCH * CHUNK_LANES
LAG = 2
ORDER = [7, 6, 5, 4, 3, 2, 1, 0]


def pos(c):
    return (c % 2) * 4 + c // 2


def dot(a, b):
    return lax.dot_general(a, b, (((1,), (0,)), ((), ())), precision=HI, preferred_element_type=F32)


def dot_nt(a, b):
    return lax.dot_general(a, b, (((1,), (1,)), ((), ())), precision=HI, preferred_element_type=F32)


def aligned(i, m=128):
    return pl.multiple_of(i * m, m)


def body(p_ref, t_ref, z_ref, out_ref, g_ref, stage, tblk, xt, gv, w_acc, s_acc, ybuf, yout, own_sem, in_sem, tile_sem, recv, send, ysem):
    z = lax.axis_index("row")
    c = lax.axis_index("col")
    xb = (c // 2) % 2
    yb = c // 4
    kb = c % 2
    steps = {"x": (2 - 4 * xb, 0), "y": (4 - 8 * yb, 0), "z": (0, 1 - 2 * z)}

    def device(dims):
        return z + sum(steps[d][1] for d in dims), c + sum(steps[d][0] for d in dims)

    def row_of(dims):
        zz, cc = device(dims)
        return pl.multiple_of(zz * 256 + ((cc % 2) * 4 + cc // 2) * 32, 32)

    partner = (z, c + 1 - 2 * kb)
    subsets = ["", "x", "y", "z", "xy", "yz", "xz", "xyz"]
    rows = {frozenset(s): row_of(s) for s in subsets}
    neigh = {d: device(d) for d in "xyz"}
    own = rows[frozenset()]

    barrier = pltpu.get_barrier_semaphore()
    for dev in (neigh["x"], neigh["y"], neigh["z"], partner):
        pl.semaphore_signal(barrier, inc=1, device_id=dev, device_id_type=MESH)
    pl.semaphore_wait(barrier, 4)

    ld_own = pltpu.make_async_copy(p_ref, stage, own_sem.at[0])
    ld_own.start()
    ld_z = pltpu.make_async_copy(z_ref, yout, in_sem.at[0])
    ld_z.start()
    ld_t = pltpu.make_async_copy(t_ref, tblk, in_sem.at[1])
    ld_t.start()

    def push(stg, chunk, sources, part, dim, first=False):
        lo = pl.multiple_of(chunk * CHUNK_LANES + part * PART_LANES, 128)
        for s in sources:
            row = rows[frozenset(s)]
            src = p_ref.at[:, pl.ds(lo, PART_LANES)] if first else g_ref.at[pl.ds(row, PW), pl.ds(lo, PART_LANES)]
            pltpu.make_async_remote_copy(
                src_ref=src,
                dst_ref=g_ref.at[pl.ds(row, PW), pl.ds(lo, PART_LANES)],
                send_sem=send.at[stg],
                recv_sem=recv.at[stg, chunk],
                device_id=neigh[dim],
                device_id_type=MESH,
            ).start()

    def wait_in(stg, chunk):
        n = PW * (1, 2, 4, 8)[stg]
        ref = g_ref.at[pl.ds(0, n), pl.ds(aligned(chunk, CHUNK_LANES), CHUNK_LANES)]
        pltpu.make_async_copy(ref, ref, recv.at[stg, chunk]).wait()

    rots = ["xyz", "yzx", "zxy"]

    def comm_step(i, _):
        @pl.when((i >= 3 * LAG) & (i < NCH + 3 * LAG))
        def _():
            ch = i - 3 * LAG
            wait_in(2, ch)
            for s in subsets:
                row = rows[frozenset(s)]
                ref = g_ref.at[pl.ds(row, PW), pl.ds(aligned(ch, CHUNK_LANES), CHUNK_LANES)]
                pltpu.make_async_remote_copy(
                    src_ref=ref, dst_ref=ref, send_sem=send.at[3], recv_sem=recv.at[3, ch], device_id=partner, device_id_type=MESH
                ).start()

        @pl.when((i >= 2 * LAG) & (i < NCH + 2 * LAG))
        def _():
            ch = i - 2 * LAG
            wait_in(1, ch)
            for p, r in enumerate(rots):
                push(2, ch, ["", r[0], r[1], r[0] + r[1]], p, r[2])

        @pl.when((i >= LAG) & (i < NCH + LAG))
        def _():
            ch = i - LAG
            wait_in(0, ch)
            for p, r in enumerate(rots):
                push(1, ch, ["", r[0]], p, r[1])

        @pl.when(i < NCH)
        def _():
            for p, r in enumerate(rots):
                push(0, i, [""], p, r[0], first=True)

        return 0

    def comm(lo, hi):
        lax.fori_loop(lo, hi, comm_step, 0)

    comm(0, LAG)
    ld_own.wait()
    st_own = pltpu.make_async_copy(stage, g_ref.at[pl.ds(own, PW), :], own_sem.at[1])
    st_own.start()
    st_own.wait()
    comm(LAG, 2 * LAG)

    ld_z.wait()

    def make_xt(b, _):
        for h in range(2):
            xt[b, :, h * 128 : (h + 1) * 128] = yout[h * NR + b].T
        return 0

    lax.fori_loop(0, NR, make_xt, 0)
    ld_t.wait()

    def tiles_before(t):
        ph = t // NR
        u = t % NR
        return ph * NTILE + u * (u + 1) // 2

    def chunks_for(t):
        return (tiles_before(t + 1) + CHUNK_TILES - 1) // CHUNK_TILES

    def steps_for(t):
        return jnp.minimum(chunks_for(t) + 3 * LAG, NCH + 3 * LAG)

    def fetch(t):
        slot = t % 2
        base = tiles_before(t)

        def one(j, _):
            for h in range(2):
                pltpu.make_async_copy(
                    g_ref.at[pl.ds(256 * h, 256), pl.ds(aligned(base + j), 128)],
                    gv.at[slot, j, :, pl.ds(128 * h, 128)],
                    tile_sem.at[slot, j],
                ).start()
            return 0

        lax.fori_loop(0, t % NR + 1, one, 0)

    def tile_wait(slot, j):
        pltpu.make_async_copy(gv.at[slot, j], gv.at[slot, j], tile_sem.at[slot, j]).wait()

    def arrive(t, prev):
        def one(ch, _):
            wait_in(3, ch)
            return 0

        lax.fori_loop(prev, chunks_for(t), one, 0)

    def eliminate(a_s, a_w):
        ybuf[...] = jnp.zeros_like(ybuf)
        for n, cc in enumerate(ORDER):
            q = pos(cc) * 32
            y = a_w[q : q + 32]
            if n:
                y = y - dot(a_s[q : q + 32], ybuf[...])
            ybuf[q : q + 32, :] = y

    def prefetch(t):
        @pl.when(t + 1 < 2 * NR)
        def _():
            comm(steps_for(t), steps_for(t + 1))
            arrive(t + 1, chunks_for(t))
            fetch(t + 1)

    comm(2 * LAG, steps_for(0))
    arrive(0, 0)
    fetch(0)

    def house(t, _):
        r = NR - 1 - t
        slot = t % 2
        prefetch(t)
        w_acc[...] = jnp.zeros_like(w_acc)
        s_acc[...] = jnp.zeros_like(s_acc)

        def gather(j, _):
            tile_wait(slot, j)
            g = gv[slot, j]
            w_acc[...] += dot_nt(xt[r + j], g)
            s_acc[...] += dot_nt(g, g)
            return 0

        lax.fori_loop(0, t + 1, gather, 0)
        tb = tblk[r]
        eliminate(dot(tb, s_acc[...]), dot(tb, w_acc[...].T))
        yt = ybuf[...].T

        def scatter(j, _):
            xt[r + j] -= dot(yt, gv[slot, j])
            return 0

        lax.fori_loop(0, t + 1, scatter, 0)
        return 0

    lax.fori_loop(0, NR, house, 0)

    row_ids = lax.broadcasted_iota(jnp.int32, (256, 256), 0) // 32
    col_ids = lax.broadcasted_iota(jnp.int32, (256, 256), 1) // 32
    other = neigh["z"]

    def solve(u, _):
        t = NR + u
        r = NR - 1 - u
        slot = t % 2
        prefetch(t)
        w_acc[...] = xt[r]
        tile_wait(slot, 0)

        def gather(j, _):
            tile_wait(slot, j)
            w_acc[...] -= dot_nt(xt[r + j], gv[slot, j])
            return 0

        lax.fori_loop(1, u + 1, gather, 0)
        d = gv[slot, 0]
        tb = jnp.where(row_ids == col_ids, d, 0.0)
        eliminate(dot(tb, d), dot(tb, w_acc[...].T))
        y = ybuf[...]
        yout[2 * r] = y[:128]
        yout[2 * r + 1] = y[128:]
        xt[r] = y.T
        dst = out_ref.at[pl.ds(aligned(r), 128), pl.ds(aligned(z), 128)]
        pltpu.make_async_copy(yout.at[2 * r + z], dst, ysem.at[0]).start()
        pltpu.make_async_remote_copy(
            src_ref=yout.at[2 * r + 1 - z], dst_ref=dst, send_sem=ysem.at[1], recv_sem=ysem.at[2], device_id=other, device_id_type=MESH
        ).start()
        return 0

    lax.fori_loop(0, NR, solve, 0)
    half = out_ref.at[:, pl.ds(0, 128)]
    for i in range(3):
        pltpu.make_async_copy(half, half, ysem.at[i]).wait()
    for stg, n in enumerate((1, 2, 4, 8)):
        ref = g_ref.at[pl.ds(0, n * PW), :]
        pltpu.make_async_copy(ref, ref, send.at[stg]).wait()


def back_transform(p, tblk, z):
    any_spec = pl.BlockSpec(memory_space=pl.ANY)
    return pl.pallas_call(
        body,
        out_shape=(jax.ShapeDtypeStruct((2048, 256), F32), jax.ShapeDtypeStruct((512, LANES), F32)),
        in_specs=[any_spec] * 3,
        out_specs=(any_spec, any_spec),
        scratch_shapes=[
            pltpu.VMEM((PW, LANES), F32),
            pltpu.VMEM((NR, 256, 256), F32),
            pltpu.VMEM((NR, 128, 256), F32),
            pltpu.VMEM((2, NR, 256, 256), F32),
            pltpu.VMEM((128, 256), F32),
            pltpu.VMEM((256, 256), F32),
            pltpu.VMEM((256, 128), F32),
            pltpu.VMEM((2 * NR, 128, 128), F32),
            pltpu.SemaphoreType.DMA((2,)),
            pltpu.SemaphoreType.DMA((2,)),
            pltpu.SemaphoreType.DMA((2, NR)),
            pltpu.SemaphoreType.DMA((4, NCH)),
            pltpu.SemaphoreType.DMA((4,)),
            pltpu.SemaphoreType.DMA((3,)),
        ],
        compiler_params=pltpu.CompilerParams(collective_id=0, has_side_effects=True, vmem_limit_bytes=60 << 20),
        name="back_transform",
    )(p, tblk, z)


def local_work(v_loc, t_all, z_loc, l_loc):
    c = lax.axis_index("col")
    z = lax.axis_index("row")
    t_pan = t_all.reshape(NR, 4, 2, PW, PW).transpose(0, 2, 1, 3, 4).reshape(NR, 8, PW, PW)
    tblk = (t_pan[:, :, :, None, :] * jnp.eye(8, dtype=F32)[None, :, None, :, None]).reshape(NR, 256, 256)

    lt = l_loc.T
    sub = (c // 2) * PW
    diag = jnp.stack([lax.dynamic_slice(l_loc, (128 * r + sub, PW * r), (PW, PW)) for r in range(NR)])
    eye = jnp.broadcast_to(jnp.eye(PW, dtype=F32), diag.shape)
    mine = (c % 2) == z
    diag = jnp.where(mine, diag, eye)
    inv_t = jnp.swapaxes(lax.linalg.triangular_solve(diag, eye, left_side=True, lower=True), 1, 2)

    def stream(mat):
        return [mat[PW * r : PW * (r + 1), 128 * r :] for r in range(NR - 1, -1, -1)]

    l_parts = []
    for r in range(NR - 1, -1, -1):
        strip = lt[PW * r : PW * (r + 1), 128 * r :]
        first = strip[:, :128]
        first = jnp.where(mine, lax.dynamic_update_slice(first, inv_t[r], (0, sub)), first)
        l_parts.append(first)
        if r < NR - 1:
            l_parts.append(strip[:, 128:])
    pad = jnp.zeros((PW, LANES - 2 * NTILE * 128), F32)
    p = jnp.concatenate(stream(v_loc.T) + l_parts + [pad], axis=1)
    y, _ = back_transform(p, tblk, z_loc.reshape(2 * NR, 128, 128))
    return y


def solution(mesh):
    return jax.shard_map(
        local_work,
        mesh=mesh,
        in_specs=(P("row", "col"), P(), P(None, ("col", "row")), P("row", "col")),
        out_specs=P("row", "col"),
        check_vma=False,
    )
```

```python
import functools

import jax
import jax.numpy as jnp
from jax import lax
from jax.experimental import pallas as pl
from jax.experimental.pallas import tpu as pltpu
from jax.sharding import PartitionSpec as P

HI = lax.Precision.HIGHEST
MESH = pl.DeviceIdType.MESH
F32 = jnp.float32

PW = 32
NR = 16
NTILE = NR * (NR + 1) // 2
PARTS = 3
PART_LANES = 256
CHUNK_TILES = PARTS * PART_LANES // 128
CHUNK_LANES = CHUNK_TILES * 128
NCH = -(-2 * NTILE // CHUNK_TILES)
LANES = NCH * CHUNK_LANES
LAG = 2
FIXED, GATHER, SCATTER, SOLVE = 30, 6, 3, 3
TOTAL_COST = 2 * NR * FIXED + NTILE * (GATHER + SCATTER + SOLVE)
ORDER = [7, 6, 5, 4, 3, 2, 1, 0]


def pos(c):
    return (c % 2) * 4 + c // 2


def dot(a, b):
    return lax.dot_general(a, b, (((1,), (0,)), ((), ())), precision=HI, preferred_element_type=F32)


def dot_nt(a, b):
    return lax.dot_general(a, b, (((1,), (1,)), ((), ())), precision=HI, preferred_element_type=F32)


def aligned(i, m=128):
    return pl.multiple_of(i * m, m)


def body(v_ref, l_ref, t_ref, z_ref, out_ref, g_ref, vin, lin, stage, tin, tb, xt, gv, w_acc, s_acc, ybuf, yout, own_sem, in_sem, tile_sem, recv, send, ysem):
    z = lax.axis_index("row")
    c = lax.axis_index("col")
    xb = (c // 2) % 2
    yb = c // 4
    kb = c % 2
    steps = {"x": (2 - 4 * xb, 0), "y": (4 - 8 * yb, 0), "z": (0, 1 - 2 * z)}

    def device(dims):
        return z + sum(steps[d][1] for d in dims), c + sum(steps[d][0] for d in dims)

    def row_of(dims):
        zz, cc = device(dims)
        return pl.multiple_of(zz * 256 + ((cc % 2) * 4 + cc // 2) * 32, 32)

    partner = (z, c + 1 - 2 * kb)
    subsets = ["", "x", "y", "z", "xy", "yz", "xz", "xyz"]
    rows = {frozenset(s): row_of(s) for s in subsets}
    neigh = {d: device(d) for d in "xyz"}
    own = rows[frozenset()]

    loads = {}
    for n, (ref, dst) in enumerate(((v_ref, vin), (l_ref, lin))):
        for cg in (3, 2, 1, 0):
            part = (pl.ds(512 * cg, 2048 - 512 * cg), pl.ds(128 * cg, 128))
            loads[n, cg] = pltpu.make_async_copy(ref.at[part], dst.at[part], in_sem.at[4 * n + cg])
            loads[n, cg].start()
    ld_z = pltpu.make_async_copy(z_ref, yout, in_sem.at[8])
    ld_z.start()
    ld_t = pltpu.make_async_copy(t_ref, tin, in_sem.at[9])
    ld_t.start()

    barrier = pltpu.get_barrier_semaphore()
    for dev in (neigh["x"], neigh["y"], neigh["z"], partner):
        pl.semaphore_signal(barrier, inc=1, device_id=dev, device_id_type=MESH)
    pl.semaphore_wait(barrier, 4)

    def push(stg, chunk, sources, part, dim):
        lo = pl.multiple_of(chunk * CHUNK_LANES + part * PART_LANES, 128)
        for s in sources:
            row = rows[frozenset(s)]
            dst = g_ref.at[pl.ds(row, PW), pl.ds(lo, PART_LANES)]
            pltpu.make_async_remote_copy(
                src_ref=dst if s else stage.at[:, pl.ds(lo, PART_LANES)],
                dst_ref=dst,
                send_sem=send.at[stg],
                recv_sem=recv.at[stg, chunk],
                device_id=neigh[dim],
                device_id_type=MESH,
            ).start()

    def wait_in(stg, chunk):
        n = PW * (1, 2, 4, 8)[stg]
        ref = g_ref.at[pl.ds(0, n), pl.ds(aligned(chunk, CHUNK_LANES), CHUNK_LANES)]
        pltpu.make_async_copy(ref, ref, recv.at[stg, chunk]).wait()

    rots = ["xyz", "yzx", "zxy"]

    def comm_step(i, _):
        @pl.when((i >= 3 * LAG) & (i < NCH + 3 * LAG))
        def _():
            ch = i - 3 * LAG
            wait_in(2, ch)
            lanes = pl.ds(aligned(ch, CHUNK_LANES), CHUNK_LANES)
            for s in subsets:
                dst = g_ref.at[pl.ds(rows[frozenset(s)], PW), lanes]
                pltpu.make_async_remote_copy(
                    src_ref=dst if s else stage.at[:, lanes],
                    dst_ref=dst,
                    send_sem=send.at[3],
                    recv_sem=recv.at[3, ch],
                    device_id=partner,
                    device_id_type=MESH,
                ).start()

        @pl.when((i >= 2 * LAG) & (i < NCH + 2 * LAG))
        def _():
            ch = i - 2 * LAG
            wait_in(1, ch)
            for p, r in enumerate(rots):
                push(2, ch, ["", r[0], r[1], r[0] + r[1]], p, r[2])

        @pl.when((i >= LAG) & (i < NCH + LAG))
        def _():
            ch = i - LAG
            wait_in(0, ch)
            for p, r in enumerate(rots):
                push(1, ch, ["", r[0]], p, r[1])

        @pl.when(i < NCH)
        def _():
            for p, r in enumerate(rots):
                push(0, i, [""], p, r[0])

        return 0

    def comm(lo, hi):
        lax.fori_loop(lo, hi, comm_step, 0)

    def tile_index(base, r, b):
        t = NR - 1 - r
        return base + t * (t + 1) // 2 + b - r

    def pack(src, base, cg):
        def block(b, rounds):
            x = src[pl.ds(aligned(b), 128), 128 * cg : 128 * cg + 128].T
            for i in rounds:
                stage[:, pl.ds(aligned(tile_index(base, 4 * cg + i, b)), 128)] = x[PW * i : PW * (i + 1)]

        for i in range(4):
            block(4 * cg + i, range(i + 1))

        def rest(b, _):
            block(b, range(4))
            return 0

        lax.fori_loop(4 * cg + 4, NR, rest, 0)

    for cg in (3, 2, 1, 0):
        loads[0, cg].wait()
        pack(vin, 0, cg)
        if cg == 3:
            comm(0, 1)
        elif cg == 2:
            comm(1, 2)
    stage[:, 2 * NTILE * 128 :] = jnp.zeros((PW, LANES - 2 * NTILE * 128), F32)
    v_lanes = pl.ds(0, NTILE * 128)
    st_v = pltpu.make_async_copy(stage.at[:, v_lanes], g_ref.at[pl.ds(own, PW), v_lanes], own_sem.at[0])
    st_v.start()
    comm(2, 3)
    for cg in (3, 2, 1, 0):
        loads[1, cg].wait()
        pack(lin, NTILE, cg)
    comm(3, 4)

    row_ids = lax.broadcasted_iota(jnp.int32, (256, 256), 0)
    col_ids = lax.broadcasted_iota(jnp.int32, (256, 256), 1)
    lane_blk = lax.broadcasted_iota(jnp.int32, (PW, 128), 1) // PW

    mine = kb == z
    sub = c // 2

    def move(x, to):
        out = x
        for a in range(4):
            shift = (to - a) * PW % 128
            out = jnp.where(sub == a, pltpu.roll(x, shift, 1) if shift else x, out)
        return out

    def invert(half, _):
        s_acc[...] = jnp.zeros_like(s_acc)

        def first(rr):
            r = half * 8 + rr
            return stage.at[:, pl.ds(aligned(tile_index(NTILE, r, r)), 128)]

        for rr in range(8):
            blk = jnp.where(lane_blk == rr % 4, move(first(rr)[...], rr % 4), 0.0)
            s_acc[PW * rr : PW * (rr + 1), rr // 4 * 128 : rr // 4 * 128 + 128] = blk
        eye = row_ids == col_ids
        u = jnp.where(mine, s_acc[...], jnp.where(eye, 1.0, 0.0))
        m = jnp.where(eye, 1.0 / jnp.where(eye, u, 1.0), 0.0)
        for s in (1, 2, 4, 8, 16):
            pair = (row_ids // (2 * s) == col_ids // (2 * s)) & (row_ids // s != col_ids // s)
            m = m - dot(m, dot(jnp.where(pair, u, 0.0), m))
        s_acc[...] = m
        for rr in range(8):
            x = s_acc[PW * rr : PW * (rr + 1), rr // 4 * 128 : rr // 4 * 128 + 128]
            back = x
            for a in range(4):
                shift = (a - rr % 4) * PW % 128
                back = jnp.where(sub == a, pltpu.roll(x, shift, 1) if shift else x, back)
            ref = first(rr)
            ref[...] = jnp.where((lane_blk == sub) & mine, back, ref[...])
        return 0

    lax.fori_loop(0, 2, lambda h, x: (invert(h, x), comm(4 + h, 5 + h))[0], 0)
    l_lanes = pl.ds(NTILE * 128, LANES - NTILE * 128)
    st_l = pltpu.make_async_copy(stage.at[:, l_lanes], g_ref.at[pl.ds(own, PW), l_lanes], own_sem.at[1])
    st_l.start()

    ld_z.wait()

    def make_xt(b, _):
        for h in range(2):
            xt[b, :, h * 128 : (h + 1) * 128] = yout[h * NR + b].T
        return 0

    lax.fori_loop(0, NR, make_xt, 0)
    ld_t.wait()
    tb[...] = jnp.zeros_like(tb)

    def tiles_before(t):
        ph = t // NR
        u = t % NR
        return ph * NTILE + u * (u + 1) // 2

    def chunks_for(t):
        return (tiles_before(t + 1) + CHUNK_TILES - 1) // CHUNK_TILES

    def paced(spent):
        return 3 * LAG + 1 + spent * NCH // TOTAL_COST

    def due(t, spent):
        return jnp.minimum(jnp.maximum(chunks_for(t) + 3 * LAG, paced(spent)), NCH + 3 * LAG)

    def fetch(t):
        slot = t % 2
        base = tiles_before(t)

        def one(j, _):
            for h in range(2):
                pltpu.make_async_copy(
                    g_ref.at[pl.ds(256 * h, 256), pl.ds(aligned(base + j), 128)],
                    gv.at[slot, j, :, pl.ds(128 * h, 128)],
                    tile_sem.at[slot, j],
                ).start()
            return 0

        lax.fori_loop(0, t % NR + 1, one, 0)

    def tile_wait(slot, j):
        pltpu.make_async_copy(gv.at[slot, j], gv.at[slot, j], tile_sem.at[slot, j]).wait()

    def arrive(t, prev):
        def one(ch, _):
            wait_in(3, ch)
            return 0

        lax.fori_loop(prev, chunks_for(t), one, 0)

    def eliminate(a_s, a_w):
        ybuf[...] = jnp.zeros_like(ybuf)
        for n, cc in enumerate(ORDER):
            q = pos(cc) * 32
            y = a_w[q : q + 32]
            if n:
                y = y - dot(a_s[q : q + 32], ybuf[...])
            ybuf[q : q + 32, :] = y

    def h_cost(t):
        return FIXED * t + (GATHER + SCATTER) * (t * (t + 1) // 2)

    def l_cost(u):
        return h_cost(NR) + FIXED * u + SOLVE * (u * (u + 1) // 2)

    def prefetch(t):
        @pl.when(t + 1 < 2 * NR)
        def _():
            arrive(t + 1, chunks_for(t))
            fetch(t + 1)

    st_v.wait()
    comm(6, due(0, 0))
    arrive(0, 0)
    fetch(0)
    st_l.wait()

    def house(t, _):
        r = NR - 1 - t
        slot = t % 2
        n = t + 1
        mid = n // 2
        c0 = h_cost(t)
        c1 = c0 + GATHER * mid
        c2 = c0 + GATHER * n + FIXED
        comm(jnp.where(t == 0, due(0, 0), due(t, c0)), due(t + 1, c0))
        prefetch(t)
        w_acc[...] = jnp.zeros_like(w_acc)
        s_acc[...] = jnp.zeros_like(s_acc)

        def gather(j, _):
            tile_wait(slot, j)
            g = gv[slot, j]
            w_acc[...] += dot_nt(xt[r + j], g)
            s_acc[...] += dot_nt(g, g)
            return 0

        lax.fori_loop(0, mid, gather, 0)
        comm(due(t + 1, c0), due(t + 1, c1))
        lax.fori_loop(mid, n, gather, 0)
        for cc in range(8):
            q = pos(cc)
            x = tin[8 * r + cc]
            x = jnp.concatenate([x] * 4, axis=1)
            tb[PW * q : PW * (q + 1), q // 4 * 128 : q // 4 * 128 + 128] = jnp.where(lane_blk == q % 4, x, 0.0)
        tbv = tb[...]
        eliminate(dot(tbv, s_acc[...]), dot(tbv, w_acc[...].T))
        yt = ybuf[...].T
        comm(due(t + 1, c1), due(t + 1, c2))

        def scatter(j, _):
            xt[r + j] -= dot(yt, gv[slot, j])
            return 0

        lax.fori_loop(0, n, scatter, 0)
        comm(due(t + 1, c2), due(t + 1, h_cost(t + 1)))
        return 0

    lax.fori_loop(0, NR, house, 0)

    other = neigh["z"]

    def solve(u, _):
        t = NR + u
        r = NR - 1 - u
        slot = t % 2
        comm(due(t, l_cost(u)), due(t + 1, l_cost(u)))
        prefetch(t)
        w_acc[...] = xt[r]
        tile_wait(slot, 0)

        def gather(j, _):
            tile_wait(slot, j)
            w_acc[...] -= dot_nt(xt[r + j], gv[slot, j])
            return 0

        lax.fori_loop(1, u + 1, gather, 0)
        d = gv[slot, 0]
        tbv = jnp.where(row_ids // PW == col_ids // PW, d, 0.0)
        eliminate(dot(tbv, d), dot(tbv, w_acc[...].T))
        y = ybuf[...]
        yout[2 * r] = y[:128]
        yout[2 * r + 1] = y[128:]
        xt[r] = y.T
        comm(due(t + 1, l_cost(u)), due(t + 1, l_cost(u + 1)))
        dst = out_ref.at[pl.ds(aligned(r), 128), pl.ds(aligned(z), 128)]
        pltpu.make_async_copy(yout.at[2 * r + z], dst, ysem.at[0]).start()
        pltpu.make_async_remote_copy(
            src_ref=yout.at[2 * r + 1 - z], dst_ref=dst, send_sem=ysem.at[1], recv_sem=ysem.at[2], device_id=other, device_id_type=MESH
        ).start()
        return 0

    lax.fori_loop(0, NR, solve, 0)
    half = out_ref.at[:, pl.ds(0, 128)]
    for i in range(3):
        pltpu.make_async_copy(half, half, ysem.at[i]).wait()
    for stg, n in enumerate((1, 2, 4, 8)):
        ref = g_ref.at[pl.ds(0, n * PW), :]
        pltpu.make_async_copy(ref, ref, send.at[stg]).wait()


def back_transform(v, l, t, z):
    any_spec = pl.BlockSpec(memory_space=pl.ANY)
    return pl.pallas_call(
        body,
        out_shape=(jax.ShapeDtypeStruct((2048, 256), F32), jax.ShapeDtypeStruct((512, LANES), F32)),
        in_specs=[any_spec] * 4,
        out_specs=(any_spec, any_spec),
        scratch_shapes=[
            pltpu.VMEM((2048, 512), F32),
            pltpu.VMEM((2048, 512), F32),
            pltpu.VMEM((PW, LANES), F32),
            pltpu.VMEM((8 * NR, PW, PW), F32),
            pltpu.VMEM((256, 256), F32),
            pltpu.VMEM((NR, 128, 256), F32),
            pltpu.VMEM((2, NR, 256, 256), F32),
            pltpu.VMEM((128, 256), F32),
            pltpu.VMEM((256, 256), F32),
            pltpu.VMEM((256, 128), F32),
            pltpu.VMEM((2 * NR, 128, 128), F32),
            pltpu.SemaphoreType.DMA((2,)),
            pltpu.SemaphoreType.DMA((10,)),
            pltpu.SemaphoreType.DMA((2, NR)),
            pltpu.SemaphoreType.DMA((4, NCH)),
            pltpu.SemaphoreType.DMA((4,)),
            pltpu.SemaphoreType.DMA((3,)),
        ],
        compiler_params=pltpu.CompilerParams(collective_id=0, has_side_effects=True, vmem_limit_bytes=60 << 20),
        name="back_transform",
    )(v, l, t, z)


def local_work(v_loc, t_all, z_loc, l_loc):
    y, _ = back_transform(v_loc, l_loc, t_all, z_loc.reshape(2 * NR, 128, 128))
    return y


def solution(mesh):
    return jax.shard_map(
        local_work,
        mesh=mesh,
        in_specs=(P("row", "col"), P(), P(None, ("col", "row")), P("row", "col")),
        out_specs=P("row", "col"),
        check_vma=False,
    )
```

```python
import functools

import jax
import jax.numpy as jnp
from jax import lax
from jax.experimental import pallas as pl
from jax.experimental.pallas import tpu as pltpu
from jax.sharding import PartitionSpec as P

MESH = pl.DeviceIdType.MESH
F32 = jnp.float32

PW = 32
NR = 16
NTILE = NR * (NR + 1) // 2
PART_TILES = (3, 4, 4)
CHUNK_TILES = sum(PART_TILES)
CHUNK_LANES = CHUNK_TILES * 128
NCH = -(-2 * NTILE // CHUNK_TILES)
LANES = NCH * CHUNK_LANES
LAG = 2
LEAD = 1
WIDTH_G, WIDTH_S, WIDTH_L = 4, 4, 4
FIXED, GATHER, SCATTER, SOLVE = 23, 5, 2, 3
TOTAL_COST = 2 * NR * FIXED + NTILE * (GATHER + SCATTER + SOLVE)
ORDER = [7, 6, 5, 4, 3, 2, 1, 0]


def pos(c):
    return (c % 2) * 4 + c // 2


BF = jnp.bfloat16


def split(x):
    hi = x.astype(BF)
    rest = x - hi.astype(F32)
    mid = rest.astype(BF)
    return hi, mid, (rest - mid.astype(F32)).astype(BF)


def lhs(s):
    hi, mid, lo = s
    return jnp.concatenate([lo, hi, mid, mid, hi, hi], axis=1)


def rhs(s, axis):
    hi, mid, lo = s
    return jnp.concatenate([hi, lo, mid, hi, mid, hi], axis=axis)


def dot(a, b):
    return jnp.dot(lhs(split(a)), rhs(split(b), 0), preferred_element_type=F32)


def dot_nt_split(pairs):
    a = jnp.concatenate([lhs(p[0]) for p in pairs], axis=1)
    b = jnp.concatenate([rhs(p[1], 1) for p in pairs], axis=1)
    return lax.dot_general(a, b, (((1,), (1,)), ((), ())), preferred_element_type=F32)


def tile_loop(lo, hi, width, fn):
    full = (hi - lo) // width

    def group(i, _):
        fn([lo + width * i + k for k in range(width)])
        return 0

    def single(j, _):
        fn([j])
        return 0

    lax.fori_loop(0, full, group, 0)
    lax.fori_loop(lo + width * full, hi, single, 0)


def aligned(i, m=128):
    return pl.multiple_of(i * m, m)


def body(v_ref, l_ref, t_ref, z_ref, out_ref, g_ref, vin, lin, stage, tin, tb, xt, gv, w_acc, s_acc, acc, ybuf, ysplit, gsplit, xsplit, yout, own_sem, in_sem, tile_sem, recv, send, ysem):
    z = lax.axis_index("row")
    c = lax.axis_index("col")
    xb = (c // 2) % 2
    yb = c // 4
    kb = c % 2
    steps = {"x": (2 - 4 * xb, 0), "y": (4 - 8 * yb, 0), "z": (0, 1 - 2 * z)}

    def device(dims):
        return z + sum(steps[d][1] for d in dims), c + sum(steps[d][0] for d in dims)

    def row_of(dims):
        zz, cc = device(dims)
        return pl.multiple_of(zz * 256 + ((cc % 2) * 4 + cc // 2) * 32, 32)

    partner = (z, c + 1 - 2 * kb)
    subsets = ["", "x", "y", "z", "xy", "yz", "xz", "xyz"]
    rows = {frozenset(s): row_of(s) for s in subsets}
    neigh = {d: device(d) for d in "xyz"}
    own = rows[frozenset()]

    loads = {}
    for n, (ref, dst) in enumerate(((v_ref, vin), (l_ref, lin))):
        for cg in (3, 2, 1, 0):
            part = (pl.ds(512 * cg, 2048 - 512 * cg), pl.ds(128 * cg, 128))
            loads[n, cg] = pltpu.make_async_copy(ref.at[part], dst.at[part], in_sem.at[4 * n + cg])
            loads[n, cg].start()
    ld_z = pltpu.make_async_copy(z_ref, yout, in_sem.at[8])
    ld_z.start()
    ld_t = pltpu.make_async_copy(t_ref, tin, in_sem.at[9])
    ld_t.start()

    barrier = pltpu.get_barrier_semaphore()
    for dev in (neigh["x"], neigh["y"], neigh["z"], partner):
        pl.semaphore_signal(barrier, inc=1, device_id=dev, device_id_type=MESH)
    pl.semaphore_wait(barrier, 4)

    def push(stg, chunk, sources, part, dim):
        lo = pl.multiple_of(chunk * CHUNK_LANES + sum(PART_TILES[:part]) * 128, 128)
        lanes = pl.ds(lo, PART_TILES[part] * 128)
        for s in sources:
            row = rows[frozenset(s)]
            dst = g_ref.at[pl.ds(row, PW), lanes]
            pltpu.make_async_remote_copy(
                src_ref=dst if s else stage.at[:, lanes],
                dst_ref=dst,
                send_sem=send.at[stg],
                recv_sem=recv.at[stg, chunk],
                device_id=neigh[dim],
                device_id_type=MESH,
            ).start()

    def wait_in(stg, chunk):
        n = PW * (1, 2, 4, 8)[stg]
        ref = g_ref.at[pl.ds(0, n), pl.ds(aligned(chunk, CHUNK_LANES), CHUNK_LANES)]
        pltpu.make_async_copy(ref, ref, recv.at[stg, chunk]).wait()

    rots = ["xyz", "yzx", "zxy"]

    def comm_step(i, _):
        @pl.when((i >= 3 * LAG) & (i < NCH + 3 * LAG))
        def _():
            ch = i - 3 * LAG
            wait_in(2, ch)
            lanes = pl.ds(aligned(ch, CHUNK_LANES), CHUNK_LANES)
            for s in subsets:
                dst = g_ref.at[pl.ds(rows[frozenset(s)], PW), lanes]
                pltpu.make_async_remote_copy(
                    src_ref=dst if s else stage.at[:, lanes],
                    dst_ref=dst,
                    send_sem=send.at[3],
                    recv_sem=recv.at[3, ch],
                    device_id=partner,
                    device_id_type=MESH,
                ).start()

        @pl.when((i >= 2 * LAG) & (i < NCH + 2 * LAG))
        def _():
            ch = i - 2 * LAG
            wait_in(1, ch)
            for p, r in enumerate(rots):
                push(2, ch, ["", r[0], r[1], r[0] + r[1]], p, r[2])

        @pl.when((i >= LAG) & (i < NCH + LAG))
        def _():
            ch = i - LAG
            wait_in(0, ch)
            for p, r in enumerate(rots):
                push(1, ch, ["", r[0]], p, r[1])

        @pl.when(i < NCH)
        def _():
            for p, r in enumerate(rots):
                push(0, i, [""], p, r[0])

        return 0

    def comm(lo, hi):
        lax.fori_loop(lo, hi, comm_step, 0)

    def tile_index(base, r, b):
        t = NR - 1 - r
        return base + t * (t + 1) // 2 + b - r

    def pack(src, base, cg):
        def block(b, rounds):
            x = src[pl.ds(aligned(b), 128), 128 * cg : 128 * cg + 128].T
            for i in rounds:
                stage[:, pl.ds(aligned(tile_index(base, 4 * cg + i, b)), 128)] = x[PW * i : PW * (i + 1)]

        for i in range(4):
            block(4 * cg + i, range(i + 1))

        def rest(b, _):
            block(b, range(4))
            return 0

        lax.fori_loop(4 * cg + 4, NR, rest, 0)

    for cg in (3, 2, 1, 0):
        loads[0, cg].wait()
        pack(vin, 0, cg)
        if cg == 2:
            comm(0, 2)
    if LANES > 2 * NTILE * 128:
        stage[:, 2 * NTILE * 128 :] = jnp.zeros((PW, LANES - 2 * NTILE * 128), F32)
    v_lanes = pl.ds(0, NTILE * 128)
    st_v = pltpu.make_async_copy(stage.at[:, v_lanes], g_ref.at[pl.ds(own, PW), v_lanes], own_sem.at[0])
    st_v.start()
    comm(2, 3)
    for cg in (3, 2, 1, 0):
        loads[1, cg].wait()
        pack(lin, NTILE, cg)
    comm(3, 4)

    row_ids = lax.broadcasted_iota(jnp.int32, (256, 256), 0)
    col_ids = lax.broadcasted_iota(jnp.int32, (256, 256), 1)
    lane_blk = lax.broadcasted_iota(jnp.int32, (PW, 128), 1) // PW

    mine = kb == z
    sub = c // 2

    def move(x, to):
        out = x
        for a in range(4):
            shift = (to - a) * PW % 128
            out = jnp.where(sub == a, pltpu.roll(x, shift, 1) if shift else x, out)
        return out

    def invert(half, _):
        s_acc[...] = jnp.zeros_like(s_acc)

        def first(rr):
            r = half * 8 + rr
            return stage.at[:, pl.ds(aligned(tile_index(NTILE, r, r)), 128)]

        for rr in range(8):
            blk = jnp.where(lane_blk == rr % 4, move(first(rr)[...], rr % 4), 0.0)
            s_acc[PW * rr : PW * (rr + 1), rr // 4 * 128 : rr // 4 * 128 + 128] = blk
        eye = row_ids == col_ids
        u = jnp.where(mine, s_acc[...], jnp.where(eye, 1.0, 0.0))
        m = jnp.where(eye, 1.0 / jnp.where(eye, u, 1.0), 0.0)
        for s in (1, 2, 4, 8, 16):
            pair = (row_ids // (2 * s) == col_ids // (2 * s)) & (row_ids // s != col_ids // s)
            m = m - dot(m, dot(jnp.where(pair, u, 0.0), m))
        s_acc[...] = m
        for rr in range(8):
            x = s_acc[PW * rr : PW * (rr + 1), rr // 4 * 128 : rr // 4 * 128 + 128]
            back = x
            for a in range(4):
                shift = (a - rr % 4) * PW % 128
                back = jnp.where(sub == a, pltpu.roll(x, shift, 1) if shift else x, back)
            ref = first(rr)
            ref[...] = jnp.where((lane_blk == sub) & mine, back, ref[...])
        return 0

    lax.fori_loop(0, 2, lambda h, x: (invert(h, x), comm(4 + h, 5 + h))[0], 0)
    l_lanes = pl.ds(NTILE * 128, LANES - NTILE * 128)
    st_l = pltpu.make_async_copy(stage.at[:, l_lanes], g_ref.at[pl.ds(own, PW), l_lanes], own_sem.at[1])
    st_l.start()

    ld_z.wait()

    def make_xt(b, _):
        for h in range(2):
            xt[b, :, h * 128 : (h + 1) * 128] = yout[h * NR + b].T
        return 0

    lax.fori_loop(0, NR, make_xt, 0)
    ld_t.wait()
    tb[...] = jnp.zeros_like(tb)

    def tiles_before(t):
        ph = t // NR
        u = t % NR
        return ph * NTILE + u * (u + 1) // 2

    def chunks_for(t):
        return (tiles_before(t + 1) + CHUNK_TILES - 1) // CHUNK_TILES

    def paced(spent):
        return 3 * LAG + LEAD + spent * NCH // TOTAL_COST

    def due(t, spent):
        return jnp.minimum(jnp.maximum(jnp.maximum(chunks_for(t) + 3 * LAG + LEAD, paced(spent)), 6), NCH + 3 * LAG)

    def fetch(t):
        slot = t % 2
        base = tiles_before(t)

        def one(j, _):
            for h in range(2):
                pltpu.make_async_copy(
                    g_ref.at[pl.ds(256 * h, 256), pl.ds(aligned(base + j), 128)],
                    gv.at[slot, j, :, pl.ds(128 * h, 128)],
                    tile_sem.at[slot, j],
                ).start()
            return 0

        lax.fori_loop(0, t % NR + 1, one, 0)

    def tile_wait(slot, j):
        pltpu.make_async_copy(gv.at[slot, j], gv.at[slot, j], tile_sem.at[slot, j]).wait()

    def arrive(t, prev):
        def one(ch, _):
            wait_in(3, ch)
            return 0

        lax.fori_loop(prev, chunks_for(t), one, 0)

    def eliminate(tbv, s_mat, w_mat):
        a = dot(tbv, jnp.concatenate([s_mat, w_mat], axis=1))
        a_s = lhs(split(a[:, :256]))
        a_w = a[:, 256:]
        ysplit[...] = jnp.zeros_like(ysplit)
        for n, cc in enumerate(ORDER):
            q = pos(cc) * PW
            y = a_w[q : q + PW]
            if n:
                y = y - jnp.dot(a_s[q : q + PW], rhs([ysplit[i] for i in range(3)], 0), preferred_element_type=F32)
            ybuf[q : q + PW, :] = y
            if n < 7:
                for i, part in enumerate(split(y)):
                    ysplit[i, q : q + PW, :] = part

    def h_cost(t):
        return FIXED * t + (GATHER + SCATTER) * (t * (t + 1) // 2)

    def l_cost(u):
        return h_cost(NR) + FIXED * u + SOLVE * (u * (u + 1) // 2)

    def prefetch(t):
        @pl.when(t + 1 < 2 * NR)
        def _():
            arrive(t + 1, chunks_for(t))
            fetch(t + 1)

    st_v.wait()
    comm(6, due(0, 0))
    arrive(0, 0)
    fetch(0)
    st_l.wait()

    def house(t, _):
        r = NR - 1 - t
        slot = t % 2
        n = t + 1
        mid = n // 2 // WIDTH_G * WIDTH_G
        c0 = h_cost(t)
        c1 = c0 + GATHER * mid
        c2 = c0 + GATHER * n + FIXED
        comm(jnp.where(t == 0, due(0, 0), due(t, c0)), due(t + 1, c0))
        prefetch(t)
        acc[...] = jnp.zeros_like(acc)

        def gather(js):
            pairs = []
            for j in js:
                tile_wait(slot, j)
                gs = split(gv[slot, j])
                for i, part in enumerate(gs):
                    gsplit[j, i] = part
                pairs.append(([jnp.concatenate(p, axis=0) for p in zip(split(xt[r + j]), gs)], gs))
            acc[...] += dot_nt_split(pairs)

        tile_loop(0, mid, WIDTH_G, gather)
        comm(due(t + 1, c0), due(t + 1, c1))
        tile_loop(mid, n, WIDTH_G, gather)
        for cc in range(8):
            q = pos(cc)
            x = tin[8 * r + cc]
            x = jnp.concatenate([x] * 4, axis=1)
            tb[PW * q : PW * (q + 1), q // 4 * 128 : q // 4 * 128 + 128] = jnp.where(lane_blk == q % 4, x, 0.0)
        tbv = tb[...]
        eliminate(tbv, acc[128:], acc[:128].T)
        yt = lhs(split(ybuf[...].T))
        comm(due(t + 1, c1), due(t + 1, c2))

        def scatter(js):
            for j in js:
                xt[r + j] -= jnp.dot(yt, rhs([gsplit[j, i] for i in range(3)], 0), preferred_element_type=F32)

        tile_loop(0, n, WIDTH_S, scatter)
        comm(due(t + 1, c2), due(t + 1, h_cost(t + 1)))
        return 0

    lax.fori_loop(0, NR, house, 0)

    other = neigh["z"]

    def solve(u, _):
        t = NR + u
        r = NR - 1 - u
        slot = t % 2
        comm(due(t, l_cost(u)), due(t + 1, l_cost(u)))
        w_acc[...] = xt[r]
        tile_wait(slot, 0)

        def gather(js):
            pairs = []
            for j in js:
                tile_wait(slot, j)
                pairs.append(([xsplit[r + j, i] for i in range(3)], split(gv[slot, j])))
            w_acc[...] -= dot_nt_split(pairs)

        tile_loop(1, u + 1, WIDTH_L, gather)
        prefetch(t)
        d = gv[slot, 0]
        tbv = jnp.where(row_ids // PW == col_ids // PW, d, 0.0)
        eliminate(tbv, d, w_acc[...].T)
        y = ybuf[...]
        yout[2 * r] = y[:128]
        yout[2 * r + 1] = y[128:]
        for i, part in enumerate(split(y.T)):
            xsplit[r, i] = part
        comm(due(t + 1, l_cost(u)), due(t + 1, l_cost(u + 1)))
        dst = out_ref.at[pl.ds(aligned(r), 128), pl.ds(aligned(z), 128)]
        pltpu.make_async_copy(yout.at[2 * r + z], dst, ysem.at[0]).start()
        pltpu.make_async_remote_copy(
            src_ref=yout.at[2 * r + 1 - z], dst_ref=dst, send_sem=ysem.at[1], recv_sem=ysem.at[2], device_id=other, device_id_type=MESH
        ).start()
        return 0

    lax.fori_loop(0, NR, solve, 0)
    half = out_ref.at[:, pl.ds(0, 128)]
    for i in range(3):
        pltpu.make_async_copy(half, half, ysem.at[i]).wait()
    for stg, n in enumerate((1, 2, 4, 8)):
        ref = g_ref.at[pl.ds(0, n * PW), :]
        pltpu.make_async_copy(ref, ref, send.at[stg]).wait()


def back_transform(v, l, t, z):
    any_spec = pl.BlockSpec(memory_space=pl.ANY)
    return pl.pallas_call(
        body,
        out_shape=(jax.ShapeDtypeStruct((2048, 256), F32), jax.ShapeDtypeStruct((512, LANES), F32)),
        in_specs=[any_spec] * 4,
        out_specs=(any_spec, any_spec),
        scratch_shapes=[
            pltpu.VMEM((2048, 512), F32),
            pltpu.VMEM((2048, 512), F32),
            pltpu.VMEM((PW, LANES), F32),
            pltpu.VMEM((8 * NR, PW, PW), F32),
            pltpu.VMEM((256, 256), F32),
            pltpu.VMEM((NR, 128, 256), F32),
            pltpu.VMEM((2, NR, 256, 256), F32),
            pltpu.VMEM((128, 256), F32),
            pltpu.VMEM((256, 256), F32),
            pltpu.VMEM((384, 256), F32),
            pltpu.VMEM((256, 128), F32),
            pltpu.VMEM((3, 256, 128), BF),
            pltpu.VMEM((NR, 3, 256, 256), BF),
            pltpu.VMEM((NR, 3, 128, 256), BF),
            pltpu.VMEM((2 * NR, 128, 128), F32),
            pltpu.SemaphoreType.DMA((2,)),
            pltpu.SemaphoreType.DMA((10,)),
            pltpu.SemaphoreType.DMA((2, NR)),
            pltpu.SemaphoreType.DMA((4, NCH)),
            pltpu.SemaphoreType.DMA((4,)),
            pltpu.SemaphoreType.DMA((3,)),
        ],
        compiler_params=pltpu.CompilerParams(collective_id=0, has_side_effects=True, vmem_limit_bytes=60 << 20),
        name="back_transform",
    )(v, l, t, z)


def local_work(v_loc, t_all, z_loc, l_loc):
    y, _ = back_transform(v_loc, l_loc, t_all, z_loc.reshape(2 * NR, 128, 128))
    return y


def solution(mesh):
    return jax.shard_map(
        local_work,
        mesh=mesh,
        in_specs=(P("row", "col"), P(), P(None, ("col", "row")), P("row", "col")),
        out_specs=P("row", "col"),
        check_vma=False,
    )
```

```python
import functools

import jax
import jax.numpy as jnp
from jax import lax
from jax.experimental import pallas as pl
from jax.experimental.pallas import tpu as pltpu
from jax.sharding import PartitionSpec as P

MESH = pl.DeviceIdType.MESH
F32 = jnp.float32

PW = 32
NR = 16
NTILE = NR * (NR + 1) // 2
PART_TILES = (3, 4, 4)
CHUNK_TILES = sum(PART_TILES)
CHUNK_LANES = CHUNK_TILES * 128
NCH = -(-2 * NTILE // CHUNK_TILES)
LANES = NCH * CHUNK_LANES
LAG = 2
AHEAD = 1
LEAD = 1
WIDTH_G, WIDTH_S, WIDTH_L = 4, 4, 4
FIXED, GATHER, SCATTER, SOLVE = 46, 10, 4, 5
TOTAL_COST = 2 * NR * FIXED + NTILE * (GATHER + SCATTER + SOLVE)
ORDER = [7, 6, 5, 4, 3, 2, 1, 0]


def pos(c):
    return (c % 2) * 4 + c // 2


BF = jnp.bfloat16


def split(x):
    hi = x.astype(BF)
    rest = x - hi.astype(F32)
    mid = rest.astype(BF)
    return hi, mid, (rest - mid.astype(F32)).astype(BF)


def lhs(s):
    hi, mid, lo = s
    return jnp.concatenate([lo, hi, mid, mid, hi, hi], axis=1)


def rhs(s, axis):
    hi, mid, lo = s
    return jnp.concatenate([hi, lo, mid, hi, mid, hi], axis=axis)


def dot(a, b):
    return jnp.dot(lhs(split(a)), rhs(split(b), 0), preferred_element_type=F32)


def dot_nt_split(pairs):
    a = jnp.concatenate([lhs(p[0]) for p in pairs], axis=1)
    b = jnp.concatenate([rhs(p[1], 1) for p in pairs], axis=1)
    return lax.dot_general(a, b, (((1,), (1,)), ((), ())), preferred_element_type=F32)


def tile_loop(lo, hi, width, fn):
    full = (hi - lo) // width

    def group(i, _):
        fn([lo + width * i + k for k in range(width)])
        return 0

    def single(j, _):
        fn([j])
        return 0

    lax.fori_loop(0, full, group, 0)
    lax.fori_loop(lo + width * full, hi, single, 0)


def aligned(i, m=128):
    return pl.multiple_of(i * m, m)


def body(v_ref, l_ref, t_ref, z_ref, out_ref, g_ref, vin, lin, stage, tin, tb, xt, gv, w_acc, s_acc, acc, ybuf, ysplit, gsplit, xsplit, yout, own_sem, in_sem, tile_sem, recv, send, ysem):
    z = lax.axis_index("row")
    c = lax.axis_index("col")
    xb = (c // 2) % 2
    yb = c // 4
    kb = c % 2
    steps = {"x": (2 - 4 * xb, 0), "y": (4 - 8 * yb, 0), "z": (0, 1 - 2 * z)}

    def device(dims):
        return z + sum(steps[d][1] for d in dims), c + sum(steps[d][0] for d in dims)

    def row_of(dims):
        zz, cc = device(dims)
        return pl.multiple_of(zz * 256 + ((cc % 2) * 4 + cc // 2) * 32, 32)

    partner = (z, c + 1 - 2 * kb)
    subsets = ["", "x", "y", "z", "xy", "yz", "xz", "xyz"]
    rows = {frozenset(s): row_of(s) for s in subsets}
    neigh = {d: device(d) for d in "xyz"}
    own = rows[frozenset()]

    loads = {}
    for n, (ref, dst) in enumerate(((v_ref, vin), (l_ref, lin))):
        for cg in (3, 2, 1, 0):
            part = (pl.ds(512 * cg, 2048 - 512 * cg), pl.ds(128 * cg, 128))
            loads[n, cg] = pltpu.make_async_copy(ref.at[part], dst.at[part], in_sem.at[4 * n + cg])
            loads[n, cg].start()
    ld_z = pltpu.make_async_copy(z_ref, yout, in_sem.at[8])
    ld_z.start()
    ld_t = pltpu.make_async_copy(t_ref, tin, in_sem.at[9])
    ld_t.start()

    barrier = pltpu.get_barrier_semaphore()
    for dev in (neigh["x"], neigh["y"], neigh["z"], partner):
        pl.semaphore_signal(barrier, inc=1, device_id=dev, device_id_type=MESH)
    pl.semaphore_wait(barrier, 4)

    swap = {"x": "y", "y": "x", "z": "z"}

    def push(stg, chunk, sources, part, dim):
        odd = chunk % 2
        lo = pl.multiple_of(chunk * CHUNK_LANES + sum(PART_TILES[:part]) * 128, 128)
        lanes = pl.ds(lo, PART_TILES[part] * 128)
        (z0, c0), (z1, c1) = neigh[dim], neigh[swap[dim]]
        for s in sources:
            r0, r1 = rows[frozenset(s)], rows[frozenset(swap[d] for d in s)]
            row = r0 if r0 is r1 else pl.multiple_of(r0 + odd * (r1 - r0), 32)
            dst = g_ref.at[pl.ds(row, PW), lanes]
            pltpu.make_async_remote_copy(
                src_ref=dst if s else stage.at[:, lanes],
                dst_ref=dst,
                send_sem=send.at[stg],
                recv_sem=recv.at[stg, chunk],
                device_id=neigh[dim] if dim == "z" else (z0, c0 + odd * (c1 - c0)),
                device_id_type=MESH,
            ).start()

    def wait_in(stg, chunk):
        n = PW * (1, 2, 4, 8)[stg]
        ref = g_ref.at[pl.ds(0, n), pl.ds(aligned(chunk, CHUNK_LANES), CHUNK_LANES)]
        pltpu.make_async_copy(ref, ref, recv.at[stg, chunk]).wait()

    rots = ["xyz", "yzx", "zxy"]

    def comm_step(i, _):
        @pl.when((i >= 3 * LAG) & (i < NCH + 3 * LAG))
        def _():
            ch = i - 3 * LAG
            wait_in(2, ch)
            lanes = pl.ds(aligned(ch, CHUNK_LANES), CHUNK_LANES)
            for s in subsets:
                dst = g_ref.at[pl.ds(rows[frozenset(s)], PW), lanes]
                pltpu.make_async_remote_copy(
                    src_ref=dst if s else stage.at[:, lanes],
                    dst_ref=dst,
                    send_sem=send.at[3],
                    recv_sem=recv.at[3, ch],
                    device_id=partner,
                    device_id_type=MESH,
                ).start()

        @pl.when((i >= 2 * LAG) & (i < NCH + 2 * LAG))
        def _():
            ch = i - 2 * LAG
            wait_in(1, ch)
            for p, r in enumerate(rots):
                push(2, ch, ["", r[0], r[1], r[0] + r[1]], p, r[2])

        @pl.when((i >= LAG) & (i < NCH + LAG))
        def _():
            ch = i - LAG
            wait_in(0, ch)
            for p, r in enumerate(rots):
                push(1, ch, ["", r[0]], p, r[1])

        @pl.when(i + AHEAD < NCH)
        def _():
            first_stage(i + AHEAD)

        return 0

    def first_stage(ch):
        for p, r in enumerate(rots):
            push(0, ch, [""], p, r[0])

    def comm(lo, hi):
        lax.fori_loop(lo, hi, comm_step, 0)

    def tile_index(base, r, b):
        t = NR - 1 - r
        return base + t * (t + 1) // 2 + b - r

    def pack(src, base, cg):
        def block(b, rounds):
            x = src[pl.ds(aligned(b), 128), 128 * cg : 128 * cg + 128].T
            for i in rounds:
                stage[:, pl.ds(aligned(tile_index(base, 4 * cg + i, b)), 128)] = x[PW * i : PW * (i + 1)]

        for i in range(4):
            block(4 * cg + i, range(i + 1))

        def rest(b, _):
            block(b, range(4))
            return 0

        lax.fori_loop(4 * cg + 4, NR, rest, 0)

    for cg in (3, 2, 1, 0):
        loads[0, cg].wait()
        pack(vin, 0, cg)
        if cg == 2:
            lax.fori_loop(0, 3, lambda i, x: (first_stage(i), x)[1], 0)
        if cg == 1:
            lax.fori_loop(3, LAG + AHEAD, lambda i, x: (first_stage(i), x)[1], 0)
    if LANES > 2 * NTILE * 128:
        stage[:, 2 * NTILE * 128 :] = jnp.zeros((PW, LANES - 2 * NTILE * 128), F32)
    v_lanes = pl.ds(0, NTILE * 128)
    st_v = pltpu.make_async_copy(stage.at[:, v_lanes], g_ref.at[pl.ds(own, PW), v_lanes], own_sem.at[0])
    st_v.start()
    comm(LAG, LAG + 2)
    for cg in (3, 2, 1, 0):
        loads[1, cg].wait()
        pack(lin, NTILE, cg)
    comm(LAG + 2, LAG + 3)

    row_ids = lax.broadcasted_iota(jnp.int32, (256, 256), 0)
    col_ids = lax.broadcasted_iota(jnp.int32, (256, 256), 1)
    lane_blk = lax.broadcasted_iota(jnp.int32, (PW, 128), 1) // PW

    mine = kb == z
    sub = c // 2

    def move(x, to):
        out = x
        for a in range(4):
            shift = (to - a) * PW % 128
            out = jnp.where(sub == a, pltpu.roll(x, shift, 1) if shift else x, out)
        return out

    def invert(half, _):
        s_acc[...] = jnp.zeros_like(s_acc)

        def first(rr):
            r = half * 8 + rr
            return stage.at[:, pl.ds(aligned(tile_index(NTILE, r, r)), 128)]

        for rr in range(8):
            blk = jnp.where(lane_blk == rr % 4, move(first(rr)[...], rr % 4), 0.0)
            s_acc[PW * rr : PW * (rr + 1), rr // 4 * 128 : rr // 4 * 128 + 128] = blk
        eye = row_ids == col_ids
        u = jnp.where(mine, s_acc[...], jnp.where(eye, 1.0, 0.0))
        m = jnp.where(eye, 1.0 / jnp.where(eye, u, 1.0), 0.0)
        for s in (1, 2, 4, 8, 16):
            pair = (row_ids // (2 * s) == col_ids // (2 * s)) & (row_ids // s != col_ids // s)
            m = m - dot(m, dot(jnp.where(pair, u, 0.0), m))
        s_acc[...] = m
        for rr in range(8):
            x = s_acc[PW * rr : PW * (rr + 1), rr // 4 * 128 : rr // 4 * 128 + 128]
            back = x
            for a in range(4):
                shift = (a - rr % 4) * PW % 128
                back = jnp.where(sub == a, pltpu.roll(x, shift, 1) if shift else x, back)
            ref = first(rr)
            ref[...] = jnp.where((lane_blk == sub) & mine, back, ref[...])
        return 0

    lax.fori_loop(0, 2, lambda h, x: (invert(h, x), comm(LAG + 3 + h, LAG + 4 + h))[0], 0)
    l_lanes = pl.ds(NTILE * 128, LANES - NTILE * 128)
    st_l = pltpu.make_async_copy(stage.at[:, l_lanes], g_ref.at[pl.ds(own, PW), l_lanes], own_sem.at[1])
    st_l.start()

    ld_z.wait()

    def make_xt(b, _):
        for h in range(2):
            xt[b, :, h * 128 : (h + 1) * 128] = yout[h * NR + b].T
        return 0

    lax.fori_loop(0, NR, make_xt, 0)
    ld_t.wait()
    tb[...] = jnp.zeros_like(tb)

    def tiles_before(t):
        ph = t // NR
        u = t % NR
        return ph * NTILE + u * (u + 1) // 2

    def chunks_for(t):
        return (tiles_before(t + 1) + CHUNK_TILES - 1) // CHUNK_TILES

    def paced(spent):
        return 3 * LAG + LEAD + spent * NCH // TOTAL_COST

    def due(t, spent):
        return jnp.minimum(jnp.maximum(jnp.maximum(chunks_for(t) + 3 * LAG + LEAD, paced(spent)), LAG + 5), NCH + 3 * LAG)

    def fetch(t):
        slot = t % 2
        base = tiles_before(t)

        def one(j, _):
            for h in range(2):
                pltpu.make_async_copy(
                    g_ref.at[pl.ds(256 * h, 256), pl.ds(aligned(base + j), 128)],
                    gv.at[slot, j, :, pl.ds(128 * h, 128)],
                    tile_sem.at[slot, j],
                ).start()
            return 0

        lax.fori_loop(0, t % NR + 1, one, 0)

    def tile_wait(slot, j):
        pltpu.make_async_copy(gv.at[slot, j], gv.at[slot, j], tile_sem.at[slot, j]).wait()

    def arrive(t, prev):
        def one(ch, _):
            wait_in(3, ch)
            return 0

        lax.fori_loop(prev, chunks_for(t), one, 0)

    def eliminate(tbv, s_mat, w_mat):
        a = dot(tbv, jnp.concatenate([s_mat, w_mat], axis=1))
        a_s = lhs(split(a[:, :256]))
        a_w = a[:, 256:]
        ysplit[...] = jnp.zeros_like(ysplit)
        for n, cc in enumerate(ORDER):
            q = pos(cc) * PW
            y = a_w[q : q + PW]
            if n:
                y = y - jnp.dot(a_s[q : q + PW], rhs([ysplit[i] for i in range(3)], 0), preferred_element_type=F32)
            ybuf[q : q + PW, :] = y
            if n < 7:
                for i, part in enumerate(split(y)):
                    ysplit[i, q : q + PW, :] = part

    def h_cost(t):
        return FIXED * t + (GATHER + SCATTER) * (t * (t + 1) // 2)

    def l_cost(u):
        return h_cost(NR) + FIXED * u + SOLVE * (u * (u + 1) // 2)

    def prefetch(t):
        @pl.when(t + 1 < 2 * NR)
        def _():
            arrive(t + 1, chunks_for(t))
            fetch(t + 1)

    st_v.wait()
    comm(LAG + 5, due(0, 0))
    arrive(0, 0)
    fetch(0)
    st_l.wait()

    def house(t, _):
        r = NR - 1 - t
        slot = t % 2
        n = t + 1
        mid = n // 2 // WIDTH_G * WIDTH_G
        c0 = h_cost(t)
        c1 = c0 + GATHER * mid
        c2 = c0 + GATHER * n + FIXED
        comm(jnp.where(t == 0, due(0, 0), due(t, c0)), due(t + 1, c0))
        prefetch(t)
        acc[...] = jnp.zeros_like(acc)

        def gather(js):
            pairs = []
            for j in js:
                tile_wait(slot, j)
                gs = split(gv[slot, j])
                for i, part in enumerate(gs):
                    gsplit[j, i] = part
                pairs.append(([jnp.concatenate(p, axis=0) for p in zip(split(xt[r + j]), gs)], gs))
            acc[...] += dot_nt_split(pairs)

        tile_loop(0, mid, WIDTH_G, gather)
        comm(due(t + 1, c0), due(t + 1, c1))
        tile_loop(mid, n, WIDTH_G, gather)
        for cc in range(8):
            q = pos(cc)
            x = tin[8 * r + cc]
            x = jnp.concatenate([x] * 4, axis=1)
            tb[PW * q : PW * (q + 1), q // 4 * 128 : q // 4 * 128 + 128] = jnp.where(lane_blk == q % 4, x, 0.0)
        tbv = tb[...]
        eliminate(tbv, acc[128:], acc[:128].T)
        yt = lhs(split(ybuf[...].T))
        comm(due(t + 1, c1), due(t + 1, c2))

        def scatter(js):
            for j in js:
                xt[r + j] -= jnp.dot(yt, rhs([gsplit[j, i] for i in range(3)], 0), preferred_element_type=F32)

        tile_loop(0, n, WIDTH_S, scatter)
        comm(due(t + 1, c2), due(t + 1, h_cost(t + 1)))
        return 0

    lax.fori_loop(0, NR, house, 0)

    other = neigh["z"]

    def solve(u, _):
        t = NR + u
        r = NR - 1 - u
        slot = t % 2
        comm(due(t, l_cost(u)), due(t + 1, l_cost(u)))
        w_acc[...] = xt[r]
        tile_wait(slot, 0)

        def gather(js):
            pairs = []
            for j in js:
                tile_wait(slot, j)
                pairs.append(([xsplit[r + j, i] for i in range(3)], split(gv[slot, j])))
            w_acc[...] -= dot_nt_split(pairs)

        tile_loop(1, u + 1, WIDTH_L, gather)
        prefetch(t)
        d = gv[slot, 0]
        tbv = jnp.where(row_ids // PW == col_ids // PW, d, 0.0)
        eliminate(tbv, d, w_acc[...].T)
        y = ybuf[...]
        yout[2 * r] = y[:128]
        yout[2 * r + 1] = y[128:]
        for i, part in enumerate(split(y.T)):
            xsplit[r, i] = part
        comm(due(t + 1, l_cost(u)), due(t + 1, l_cost(u + 1)))
        dst = out_ref.at[pl.ds(aligned(r), 128), pl.ds(aligned(z), 128)]
        pltpu.make_async_copy(yout.at[2 * r + z], dst, ysem.at[0]).start()
        pltpu.make_async_remote_copy(
            src_ref=yout.at[2 * r + 1 - z], dst_ref=dst, send_sem=ysem.at[1], recv_sem=ysem.at[2], device_id=other, device_id_type=MESH
        ).start()
        return 0

    lax.fori_loop(0, NR, solve, 0)
    half = out_ref.at[:, pl.ds(0, 128)]
    for i in range(3):
        pltpu.make_async_copy(half, half, ysem.at[i]).wait()
    for stg, n in enumerate((1, 2, 4, 8)):
        ref = g_ref.at[pl.ds(0, n * PW), :]
        pltpu.make_async_copy(ref, ref, send.at[stg]).wait()


def back_transform(v, l, t, z):
    any_spec = pl.BlockSpec(memory_space=pl.ANY)
    return pl.pallas_call(
        body,
        out_shape=(jax.ShapeDtypeStruct((2048, 256), F32), jax.ShapeDtypeStruct((512, LANES), F32)),
        in_specs=[any_spec] * 4,
        out_specs=(any_spec, any_spec),
        scratch_shapes=[
            pltpu.VMEM((2048, 512), F32),
            pltpu.VMEM((2048, 512), F32),
            pltpu.VMEM((PW, LANES), F32),
            pltpu.VMEM((8 * NR, PW, PW), F32),
            pltpu.VMEM((256, 256), F32),
            pltpu.VMEM((NR, 128, 256), F32),
            pltpu.VMEM((2, NR, 256, 256), F32),
            pltpu.VMEM((128, 256), F32),
            pltpu.VMEM((256, 256), F32),
            pltpu.VMEM((384, 256), F32),
            pltpu.VMEM((256, 128), F32),
            pltpu.VMEM((3, 256, 128), BF),
            pltpu.VMEM((NR, 3, 256, 256), BF),
            pltpu.VMEM((NR, 3, 128, 256), BF),
            pltpu.VMEM((2 * NR, 128, 128), F32),
            pltpu.SemaphoreType.DMA((2,)),
            pltpu.SemaphoreType.DMA((10,)),
            pltpu.SemaphoreType.DMA((2, NR)),
            pltpu.SemaphoreType.DMA((4, NCH)),
            pltpu.SemaphoreType.DMA((4,)),
            pltpu.SemaphoreType.DMA((3,)),
        ],
        compiler_params=pltpu.CompilerParams(collective_id=0, has_side_effects=True, vmem_limit_bytes=60 << 20),
        name="back_transform",
    )(v, l, t, z)


def local_work(v_loc, t_all, z_loc, l_loc):
    y, _ = back_transform(v_loc, l_loc, t_all, z_loc.reshape(2 * NR, 128, 128))
    return y


def solution(mesh):
    return jax.shard_map(
        local_work,
        mesh=mesh,
        in_specs=(P("row", "col"), P(), P(None, ("col", "row")), P("row", "col")),
        out_specs=P("row", "col"),
        check_vma=False,
    )
```

```python
import functools

import jax
import jax.numpy as jnp
from jax import lax
from jax.experimental import pallas as pl
from jax.experimental.pallas import tpu as pltpu
from jax.sharding import PartitionSpec as P

MESH = pl.DeviceIdType.MESH
F32 = jnp.float32

PW = 32
NR = 16
NTILE = NR * (NR + 1) // 2
PART_TILES = (3, 4, 4)
CHUNK_TILES = sum(PART_TILES)
CHUNK_LANES = CHUNK_TILES * 128
NCH = -(-2 * NTILE // CHUNK_TILES)
LANES = NCH * CHUNK_LANES
LAG = 2
AHEAD = 1
LEAD = 1
WIDTH_G, WIDTH_S, WIDTH_L = 4, 4, 4
FIXED, GATHER, SCATTER, SOLVE = 46, 10, 4, 5
TOTAL_COST = 2 * NR * FIXED + NTILE * (GATHER + SCATTER + SOLVE)
ORDER = [7, 6, 5, 4, 3, 2, 1, 0]


def pos(c):
    return (c % 2) * 4 + c // 2


BF = jnp.bfloat16


def split(x):
    hi = x.astype(BF)
    rest = x - hi.astype(F32)
    mid = rest.astype(BF)
    return hi, mid, (rest - mid.astype(F32)).astype(BF)


def lhs(s):
    hi, mid, lo = s
    return jnp.concatenate([lo, hi, mid, mid, hi, hi], axis=1)


def rhs(s, axis):
    hi, mid, lo = s
    return jnp.concatenate([hi, lo, mid, hi, mid, hi], axis=axis)


def dot(a, b):
    return jnp.dot(lhs(split(a)), rhs(split(b), 0), preferred_element_type=F32)


def dot_nt_split(pairs):
    a = jnp.concatenate([lhs(p[0]) for p in pairs], axis=1)
    b = jnp.concatenate([rhs(p[1], 1) for p in pairs], axis=1)
    return lax.dot_general(a, b, (((1,), (1,)), ((), ())), preferred_element_type=F32)


def tile_loop(lo, hi, width, fn):
    full = (hi - lo) // width

    def group(i, _):
        fn([lo + width * i + k for k in range(width)])
        return 0

    def single(j, _):
        fn([j])
        return 0

    lax.fori_loop(0, full, group, 0)
    lax.fori_loop(lo + width * full, hi, single, 0)


def aligned(i, m=128):
    return pl.multiple_of(i * m, m)


def body(v_ref, l_ref, t_ref, z_ref, out_ref, g_ref, vin, lin, stage, tin, tb, xt, gv, w_acc, s_acc, acc, ybuf, ysplit, gsplit, xsplit, yout, own_sem, in_sem, tile_sem, recv, send, ysem):
    z = lax.axis_index("row")
    c = lax.axis_index("col")
    xb = (c // 2) % 2
    yb = c // 4
    kb = c % 2
    steps = {"x": (2 - 4 * xb, 0), "y": (4 - 8 * yb, 0), "z": (0, 1 - 2 * z)}

    def device(dims):
        return z + sum(steps[d][1] for d in dims), c + sum(steps[d][0] for d in dims)

    def row_of(dims):
        zz, cc = device(dims)
        return pl.multiple_of(zz * 256 + ((cc % 2) * 4 + cc // 2) * 32, 32)

    partner = (z, c + 1 - 2 * kb)
    subsets = ["", "x", "y", "z", "xy", "yz", "xz", "xyz"]
    rows = {frozenset(s): row_of(s) for s in subsets}
    neigh = {d: device(d) for d in "xyz"}
    own = rows[frozenset()]

    loads = {}
    for n, (ref, dst) in enumerate(((v_ref, vin), (l_ref, lin))):
        for cg in (3, 2, 1, 0):
            part = (pl.ds(512 * cg, 2048 - 512 * cg), pl.ds(128 * cg, 128))
            loads[n, cg] = pltpu.make_async_copy(ref.at[part], dst.at[part], in_sem.at[4 * n + cg])
            loads[n, cg].start()
    ld_z = pltpu.make_async_copy(z_ref, yout, in_sem.at[8])
    ld_z.start()
    ld_t = pltpu.make_async_copy(t_ref, tin, in_sem.at[9])
    ld_t.start()

    barrier = pltpu.get_barrier_semaphore()
    for dev in (neigh["x"], neigh["y"], neigh["z"], partner):
        pl.semaphore_signal(barrier, inc=1, device_id=dev, device_id_type=MESH)
    pl.semaphore_wait(barrier, 4)

    swap = {"x": "y", "y": "x", "z": "z"}

    def push(stg, chunk, sources, part, dim):
        odd = chunk % 2
        lo = pl.multiple_of(chunk * CHUNK_LANES + sum(PART_TILES[:part]) * 128, 128)
        lanes = pl.ds(lo, PART_TILES[part] * 128)
        (z0, c0), (z1, c1) = neigh[dim], neigh[swap[dim]]
        for s in sources:
            r0, r1 = rows[frozenset(s)], rows[frozenset(swap[d] for d in s)]
            row = r0 if r0 is r1 else pl.multiple_of(r0 + odd * (r1 - r0), 32)
            dst = g_ref.at[pl.ds(row, PW), lanes]
            pltpu.make_async_remote_copy(
                src_ref=dst if s else stage.at[:, lanes],
                dst_ref=dst,
                send_sem=send.at[stg],
                recv_sem=recv.at[stg, chunk],
                device_id=neigh[dim] if dim == "z" else (z0, c0 + odd * (c1 - c0)),
                device_id_type=MESH,
            ).start()

    def wait_in(stg, chunk):
        n = PW * (1, 2, 4, 8)[stg]
        ref = g_ref.at[pl.ds(0, n), pl.ds(aligned(chunk, CHUNK_LANES), CHUNK_LANES)]
        pltpu.make_async_copy(ref, ref, recv.at[stg, chunk]).wait()

    rots = ["xyz", "yzx", "zxy"]

    def comm_step(i, _):
        @pl.when((i >= 3 * LAG) & (i < NCH + 3 * LAG))
        def _():
            ch = i - 3 * LAG
            wait_in(2, ch)
            lanes = pl.ds(aligned(ch, CHUNK_LANES), CHUNK_LANES)
            for s in subsets:
                dst = g_ref.at[pl.ds(rows[frozenset(s)], PW), lanes]
                pltpu.make_async_remote_copy(
                    src_ref=dst if s else stage.at[:, lanes],
                    dst_ref=dst,
                    send_sem=send.at[3],
                    recv_sem=recv.at[3, ch],
                    device_id=partner,
                    device_id_type=MESH,
                ).start()

        @pl.when((i >= 2 * LAG) & (i < NCH + 2 * LAG))
        def _():
            ch = i - 2 * LAG
            wait_in(1, ch)
            for p, r in enumerate(rots):
                push(2, ch, ["", r[0], r[1], r[0] + r[1]], p, r[2])

        @pl.when((i >= LAG) & (i < NCH + LAG))
        def _():
            ch = i - LAG
            wait_in(0, ch)
            for p, r in enumerate(rots):
                push(1, ch, ["", r[0]], p, r[1])

        @pl.when(i + AHEAD < NCH)
        def _():
            first_stage(i + AHEAD)

        return 0

    def first_stage(ch):
        for p, r in enumerate(rots):
            push(0, ch, [""], p, r[0])

    def comm(lo, hi):
        lax.fori_loop(lo, hi, comm_step, 0)

    def tile_index(base, r, b):
        t = NR - 1 - r
        return base + t * (t + 1) // 2 + b - r

    def pack(src, base, cg):
        def block(b, rounds):
            x = src[pl.ds(aligned(b), 128), 128 * cg : 128 * cg + 128].T
            for i in rounds:
                stage[:, pl.ds(aligned(tile_index(base, 4 * cg + i, b)), 128)] = x[PW * i : PW * (i + 1)]

        for i in range(4):
            block(4 * cg + i, range(i + 1))

        def rest(b, _):
            block(b, range(4))
            return 0

        lax.fori_loop(4 * cg + 4, NR, rest, 0)

    for cg in (3, 2, 1, 0):
        loads[0, cg].wait()
        pack(vin, 0, cg)
        if cg == 2:
            lax.fori_loop(0, 3, lambda i, x: (first_stage(i), x)[1], 0)
        if cg == 1:
            lax.fori_loop(3, LAG + AHEAD, lambda i, x: (first_stage(i), x)[1], 0)
    if LANES > 2 * NTILE * 128:
        stage[:, 2 * NTILE * 128 :] = jnp.zeros((PW, LANES - 2 * NTILE * 128), F32)
    v_lanes = pl.ds(0, NTILE * 128)
    st_v = pltpu.make_async_copy(stage.at[:, v_lanes], g_ref.at[pl.ds(own, PW), v_lanes], own_sem.at[0])
    st_v.start()
    comm(LAG, LAG + 2)
    for cg in (3, 2, 1, 0):
        loads[1, cg].wait()
        pack(lin, NTILE, cg)
    comm(LAG + 2, LAG + 3)

    row_ids = lax.broadcasted_iota(jnp.int32, (256, 256), 0)
    col_ids = lax.broadcasted_iota(jnp.int32, (256, 256), 1)
    lane_blk = lax.broadcasted_iota(jnp.int32, (PW, 128), 1) // PW

    mine = kb == z
    sub = c // 2

    def move(x, to):
        out = x
        for a in range(4):
            shift = (to - a) * PW % 128
            out = jnp.where(sub == a, pltpu.roll(x, shift, 1) if shift else x, out)
        return out

    def invert(half, _):
        s_acc[...] = jnp.zeros_like(s_acc)

        def first(rr):
            r = half * 8 + rr
            return stage.at[:, pl.ds(aligned(tile_index(NTILE, r, r)), 128)]

        for rr in range(8):
            blk = jnp.where(lane_blk == rr % 4, move(first(rr)[...], rr % 4), 0.0)
            s_acc[PW * rr : PW * (rr + 1), rr // 4 * 128 : rr // 4 * 128 + 128] = blk
        eye = row_ids == col_ids
        u = jnp.where(mine, s_acc[...], jnp.where(eye, 1.0, 0.0))
        m = jnp.where(eye, 1.0 / jnp.where(eye, u, 1.0), 0.0)
        for s in (1, 2, 4, 8, 16):
            pair = (row_ids // (2 * s) == col_ids // (2 * s)) & (row_ids // s != col_ids // s)
            m = m - dot(m, dot(jnp.where(pair, u, 0.0), m))
        s_acc[...] = m
        for rr in range(8):
            x = s_acc[PW * rr : PW * (rr + 1), rr // 4 * 128 : rr // 4 * 128 + 128]
            back = x
            for a in range(4):
                shift = (a - rr % 4) * PW % 128
                back = jnp.where(sub == a, pltpu.roll(x, shift, 1) if shift else x, back)
            ref = first(rr)
            ref[...] = jnp.where((lane_blk == sub) & mine, back, ref[...])
        return 0

    lax.fori_loop(0, 2, lambda h, x: (invert(h, x), comm(LAG + 3 + h, LAG + 4 + h))[0], 0)
    l_lanes = pl.ds(NTILE * 128, LANES - NTILE * 128)
    st_l = pltpu.make_async_copy(stage.at[:, l_lanes], g_ref.at[pl.ds(own, PW), l_lanes], own_sem.at[1])
    st_l.start()

    ld_z.wait()

    def make_xt(b, _):
        for h in range(2):
            xt[b, :, h * 128 : (h + 1) * 128] = yout[h * NR + b].T
        return 0

    lax.fori_loop(0, NR, make_xt, 0)
    ld_t.wait()
    tb[...] = jnp.zeros_like(tb)

    def tiles_before(t):
        ph = t // NR
        u = t % NR
        return ph * NTILE + u * (u + 1) // 2

    def chunks_for(t):
        return (tiles_before(t + 1) + CHUNK_TILES - 1) // CHUNK_TILES

    def paced(spent):
        return 3 * LAG + LEAD + spent * NCH // TOTAL_COST

    def due(t, spent):
        return jnp.minimum(jnp.maximum(jnp.maximum(chunks_for(t) + 3 * LAG + LEAD, paced(spent)), LAG + 5), NCH + 3 * LAG)

    def fetch(t):
        slot = t % 2
        base = tiles_before(t)

        def one(j, _):
            for h in range(2):
                pltpu.make_async_copy(
                    g_ref.at[pl.ds(256 * h, 256), pl.ds(aligned(base + j), 128)],
                    gv.at[slot, j, :, pl.ds(128 * h, 128)],
                    tile_sem.at[slot, j],
                ).start()
            return 0

        lax.fori_loop(0, t % NR + 1, one, 0)

    def tile_wait(slot, j):
        pltpu.make_async_copy(gv.at[slot, j], gv.at[slot, j], tile_sem.at[slot, j]).wait()

    def arrive(t, prev):
        def one(ch, _):
            wait_in(3, ch)
            return 0

        lax.fori_loop(prev, chunks_for(t), one, 0)

    def eliminate(tbv, s_mat, w_mat):
        a = dot(tbv, jnp.concatenate([s_mat, w_mat], axis=1))
        a_s = lhs(split(a[:, :256]))
        a_w = a[:, 256:]
        ysplit[...] = jnp.zeros_like(ysplit)
        for n, cc in enumerate(ORDER):
            q = pos(cc) * PW
            y = a_w[q : q + PW]
            if n:
                y = y - jnp.dot(a_s[q : q + PW], rhs([ysplit[i] for i in range(3)], 0), preferred_element_type=F32)
            ybuf[q : q + PW, :] = y
            if n < 7:
                for i, part in enumerate(split(y)):
                    ysplit[i, q : q + PW, :] = part

    def h_cost(t):
        return FIXED * t + (GATHER + SCATTER) * (t * (t + 1) // 2)

    def l_cost(u):
        return h_cost(NR) + FIXED * u + SOLVE * (u * (u + 1) // 2)

    def prefetch(t):
        @pl.when(t + 1 < 2 * NR)
        def _():
            arrive(t + 1, chunks_for(t))
            fetch(t + 1)

    st_v.wait()
    comm(LAG + 5, due(0, 0))
    arrive(0, 0)
    fetch(0)
    st_l.wait()

    def house(t, _):
        r = NR - 1 - t
        slot = t % 2
        n = t + 1
        mid = n // 2 // WIDTH_G * WIDTH_G
        c0 = h_cost(t)
        c1 = c0 + GATHER * mid
        c2 = c0 + GATHER * n + FIXED
        comm(jnp.where(t == 0, due(0, 0), due(t, c0)), due(t + 1, c0))
        prefetch(t)
        acc[...] = jnp.zeros_like(acc)

        def gather(js):
            pairs = []
            for j in js:
                tile_wait(slot, j)
                gs = split(gv[slot, j])
                for i, part in enumerate(gs):
                    gsplit[j, i] = part
                pairs.append(([jnp.concatenate(p, axis=0) for p in zip(split(xt[r + j]), gs)], gs))
            acc[...] += dot_nt_split(pairs)

        tile_loop(0, mid, WIDTH_G, gather)
        comm(due(t + 1, c0), due(t + 1, c1))
        tile_loop(mid, n, WIDTH_G, gather)
        for cc in range(8):
            q = pos(cc)
            x = tin[8 * r + cc]
            x = jnp.concatenate([x] * 4, axis=1)
            tb[PW * q : PW * (q + 1), q // 4 * 128 : q // 4 * 128 + 128] = jnp.where(lane_blk == q % 4, x, 0.0)
        tbv = tb[...]
        eliminate(tbv, acc[128:], acc[:128].T)
        yt = lhs(split(ybuf[...].T))
        comm(due(t + 1, c1), due(t + 1, c2))

        def scatter(js):
            for j in js:
                xt[r + j] -= jnp.dot(yt, rhs([gsplit[j, i] for i in range(3)], 0), preferred_element_type=F32)

        tile_loop(0, n, WIDTH_S, scatter)
        comm(due(t + 1, c2), due(t + 1, h_cost(t + 1)))
        return 0

    lax.fori_loop(0, NR, house, 0)

    other = neigh["z"]

    def solve(u, _):
        t = NR + u
        r = NR - 1 - u
        slot = t % 2
        comm(due(t, l_cost(u)), due(t + 1, l_cost(u)))
        w_acc[...] = xt[r]
        tile_wait(slot, 0)

        def gather(js):
            pairs = []
            for j in js:
                tile_wait(slot, j)
                pairs.append(([xsplit[r + j, i] for i in range(3)], split(gv[slot, j])))
            w_acc[...] -= dot_nt_split(pairs)

        tile_loop(1, u + 1, WIDTH_L, gather)
        prefetch(t)
        d = gv[slot, 0]
        tbv = jnp.where(row_ids // PW == col_ids // PW, d, 0.0)
        eliminate(tbv, d, w_acc[...].T)
        y = ybuf[...]
        yout[2 * r] = y[:128]
        yout[2 * r + 1] = y[128:]
        for i, part in enumerate(split(y.T)):
            xsplit[r, i] = part
        dst = out_ref.at[pl.ds(aligned(r), 128), pl.ds(aligned(z), 128)]
        pltpu.make_async_copy(yout.at[2 * r + z], dst, ysem.at[0]).start()
        pltpu.make_async_remote_copy(
            src_ref=yout.at[2 * r + 1 - z], dst_ref=dst, send_sem=ysem.at[1], recv_sem=ysem.at[2], device_id=other, device_id_type=MESH
        ).start()
        comm(due(t + 1, l_cost(u)), due(t + 1, l_cost(u + 1)))
        return 0

    lax.fori_loop(0, NR, solve, 0)
    half = out_ref.at[:, pl.ds(0, 128)]
    for i in range(3):
        pltpu.make_async_copy(half, half, ysem.at[i]).wait()
    for stg, n in enumerate((1, 2, 4, 8)):
        ref = g_ref.at[pl.ds(0, n * PW), :]
        pltpu.make_async_copy(ref, ref, send.at[stg]).wait()


def back_transform(v, l, t, z):
    any_spec = pl.BlockSpec(memory_space=pl.ANY)
    return pl.pallas_call(
        body,
        out_shape=(jax.ShapeDtypeStruct((2048, 256), F32), jax.ShapeDtypeStruct((512, LANES), F32)),
        in_specs=[any_spec] * 4,
        out_specs=(any_spec, any_spec),
        scratch_shapes=[
            pltpu.VMEM((2048, 512), F32),
            pltpu.VMEM((2048, 512), F32),
            pltpu.VMEM((PW, LANES), F32),
            pltpu.VMEM((8 * NR, PW, PW), F32),
            pltpu.VMEM((256, 256), F32),
            pltpu.VMEM((NR, 128, 256), F32),
            pltpu.VMEM((2, NR, 256, 256), F32),
            pltpu.VMEM((128, 256), F32),
            pltpu.VMEM((256, 256), F32),
            pltpu.VMEM((384, 256), F32),
            pltpu.VMEM((256, 128), F32),
            pltpu.VMEM((3, 256, 128), BF),
            pltpu.VMEM((NR, 3, 256, 256), BF),
            pltpu.VMEM((NR, 3, 128, 256), BF),
            pltpu.VMEM((2 * NR, 128, 128), F32),
            pltpu.SemaphoreType.DMA((2,)),
            pltpu.SemaphoreType.DMA((10,)),
            pltpu.SemaphoreType.DMA((2, NR)),
            pltpu.SemaphoreType.DMA((4, NCH)),
            pltpu.SemaphoreType.DMA((4,)),
            pltpu.SemaphoreType.DMA((3,)),
        ],
        compiler_params=pltpu.CompilerParams(collective_id=0, has_side_effects=True, vmem_limit_bytes=60 << 20),
        name="back_transform",
    )(v, l, t, z)


def local_work(v_loc, t_all, z_loc, l_loc):
    y, _ = back_transform(v_loc, l_loc, t_all, z_loc.reshape(2 * NR, 128, 128))
    return y


def solution(mesh):
    return jax.shard_map(
        local_work,
        mesh=mesh,
        in_specs=(P("row", "col"), P(), P(None, ("col", "row")), P("row", "col")),
        out_specs=P("row", "col"),
        check_vma=False,
    )
```
